256 devices in a mesh: row: 8 (over y, core), col: 32 (over z, x).
Axes of the slice: x: 4, y: 4, z: 8, core: 2. Of those that a mesh axis runs over, the one named last changes fastest.
Arguments:
- rhs: bfloat16 [6144, 6144], P('row', 'col'), may hold values from -6 to 6
- basis_left: bfloat16 [6144, 6144], P('col', 'row'), may hold values from -1 to 1, as said below
- basis_right: bfloat16 [6144, 6144], P('row', 'col'), may hold values from -1 to 1, as said below
- eig_left: float32 [6144], P('row'), may hold values from 0.1 to 4
- eig_right: float32 [6144], P('col'), may hold values from 0.1 to 4
Outputs:
- solution: bfloat16 [6144, 6144], P('col', 'row')
The draws below stay inside these ranges and needn't reach their ends.
Inputs may be any that keep to these rules, and one draw needn't show every extreme that they name: `basis_left`: an orthogonal matrix drawn uniformly, rounded to bfloat16. `basis_right`: an orthogonal matrix drawn uniformly, rounded to bfloat16.
All inputs are finite; a program needn't handle non-finite values.
Results may differ from the reference program's by a relative error of at most 0.0085.
Values may be sent and summed in bfloat16 or wider, within the bound.
A program may use at most 64 MiB of HBM per device.

```python
import math
import jax
import jax.numpy as jnp

N = 6144


def orthogonal_matrix(key):
    normal_draw = jax.random.normal(key, (N, N), jnp.float32)
    factor_q, factor_r = jnp.linalg.qr(normal_draw)
    signs = jnp.where(jnp.diagonal(factor_r) < 0.0, -1.0, 1.0).astype(jnp.float32)
    return (factor_q * signs[None, :]).astype(jnp.bfloat16)


def draw_basis_left(key, part):
    return orthogonal_matrix(jax.random.fold_in(key, 11))


def draw_basis_right(key, part):
    return orthogonal_matrix(jax.random.fold_in(key, 23))


def block_levels(key, shape, pieces, smallest, top_value):
    level = 1.0
    for dim, parts in pieces:
        steps = jax.random.uniform(jax.random.fold_in(jax.random.fold_in(key, 6), dim), (parts,), jnp.float32, smallest / len(pieces), top_value / len(pieces))
        level = level * jnp.repeat(jnp.exp(steps), shape[dim] // parts).reshape((-1,) + (1,) * (len(shape) - 1 - dim))
    return level


def normal_values(own_key, extent, width, reach, cuts=(), kind=jnp.bfloat16):
    loudness = block_levels(own_key, extent, cuts, -0.22, 0.18) if cuts else 1.0
    array = jax.random.normal(own_key, extent, jnp.float32) * width * loudness
    return jnp.minimum(jnp.maximum(array, -reach), reach).astype(kind)


def setup_inputs(seed: int = 0) -> dict:
    key_list = jax.random.split(jax.random.key(seed), 6)
    return {
        "rhs": normal_values(key_list[0], (N, N), 1.0, 6.0, ((0, 8), (1, 32))),
        "basis_left": draw_basis_left(jax.random.fold_in(key_list[5], 71), 0),
        "basis_right": draw_basis_right(jax.random.fold_in(key_list[5], 71), 0),
        "eig_left": jnp.clip(jnp.exp(math.log(4.0) - 3.6888794 * jax.random.uniform(key_list[3], (N,), jnp.float32) ** block_levels(key_list[3], (N,), ((0, 8),), -0.2, 0.2)), 0.1, 4.0),
        "eig_right": jnp.clip(jnp.exp(math.log(4.0) - 3.6888794 * jax.random.uniform(key_list[4], (N,), jnp.float32) ** block_levels(key_list[4], (N,), ((0, 32),), -0.2, 0.2)), 0.1, 4.0),
    }


def reference(rhs, basis_left, basis_right, eig_left, eig_right):
    projected = jnp.dot(basis_left.T.astype(jnp.float32), rhs.astype(jnp.float32), preferred_element_type=jnp.float32).astype(jnp.bfloat16)
    second = jnp.dot(projected.astype(jnp.float32), basis_right.astype(jnp.float32), preferred_element_type=jnp.float32)
    scaled = (second / (eig_left[:, None] + eig_right[None, :])).astype(jnp.bfloat16)
    half = jnp.dot(basis_left.astype(jnp.float32), scaled.astype(jnp.float32), preferred_element_type=jnp.float32).astype(jnp.bfloat16)
    return jnp.dot(half.astype(jnp.float32), basis_right.T.astype(jnp.float32), preferred_element_type=jnp.float32).astype(jnp.bfloat16)
```

```python
import jax
import jax.numpy as jnp
from jax import lax
from jax.experimental import pallas as pl
from jax.experimental.pallas import tpu as pltpu
from jax.sharding import PartitionSpec as P

MESH = pl.DeviceIdType.MESH
B = 384
H = B // 2
Q = B // 4
R = B // 8
NX, NY, NZ = 4, 4, 8


def kernel(
    ct_ref, qa_ref, qbt_ref, el_ref, er_ref, out_ref,
    cs, qas, qbs, ps, ss, hp, hs, qb2, acc, els, ers, er_col,
    rs_t, rs_a, rs_b, rs_mid, rs_t2, rs_a2, rs_b2, h_own, xo, xin,
    swap_send, swap_recv, z_recv, xy_recv, rs_recv, fin_send, fin_recv,
    z_send, xy_send, rs_send,
):
    r, c = lax.axis_index("row"), lax.axis_index("col")
    y, core, z, x = r // 2, r % 2, c // 4, c % 4
    g1, g2 = z * 2 + core, y * 4 + x

    def dev(dx=0, dy=0, dz=0):
        return {
            "row": ((y + dy + NY) % NY) * 2 + core,
            "col": ((z + dz + NZ) % NZ) * 4 + (x + dx + NX) % NX,
        }

    sibling = {"row": y * 2 + 1 - core, "col": c}

    def remote(src, dst, send, recv, device):
        return pltpu.make_async_remote_copy(
            src_ref=src, dst_ref=dst, send_sem=send, recv_sem=recv,
            device_id=device, device_id_type=MESH,
        )

    def landed(dst, sem):
        pltpu.make_async_copy(dst, dst, sem).wait()

    barrier = pltpu.get_barrier_semaphore()
    greeted = [dev(dy=1), dev(dy=-1), dev(dz=1), dev(dz=-1), sibling]
    for dx in (1, 2, 3):
        for k in (core, 1 - core):
            greeted.append({"row": y * 2 + k, "col": z * 4 + (x + dx) % NX})
    for device in greeted:
        pl.semaphore_signal(barrier, inc=1, device_id=device, device_id_type=MESH)
    pl.semaphore_wait(barrier, len(greeted))

    half_x, odd_x = x // 2, x % 2

    def exchange(pieces, send, recv, act, only=(0, 1, 2, 3, 4), halves=(0, 1)):
        for h in halves:
            to_x = 2 * core + h
            own = jnp.logical_and(to_x == x, half_x == core)
            for n, (src, dst) in enumerate(pieces(h, to_x)):
                if n not in only:
                    continue

                @pl.when(own)
                def _(n=n, src=src, dst=dst):
                    if act == "start":
                        pltpu.make_async_copy(src, dst, recv.at[n, odd_x]).start()

                @pl.when(jnp.logical_not(own))
                def _(n=n, src=src, dst=dst, h=h, to_x=to_x):
                    copy = remote(
                        src, dst, send.at[n, h], recv.at[n, odd_x],
                        {"row": y * 2 + half_x, "col": z * 4 + to_x},
                    )
                    if act == "start":
                        copy.start()
                    else:
                        copy.wait_send()

    def first_pieces(h, to_x):
        lanes = pl.ds(h * B, B)
        rows = pl.ds(pl.multiple_of(odd_x * H, H), H)
        return (
            (qa_ref.at[:, lanes], qas.at[z * 2 + half_x, rows, :]),
            (ct_ref.at[:, lanes], cs.at[y * 4 + to_x, rows, :]),
            (qbt_ref.at[:, lanes], qbs.at[y * 4 + to_x, rows, :]),
            (el_ref.at[:, lanes], els.at[odd_x]),
            (er_ref, ers.at[odd_x]),
        )

    def first_landed(n):
        for s in (0, 1):
            rows = pl.ds(s * H, H)
            dst = (
                qas.at[g1, rows, :], cs.at[g2, rows, :], qbs.at[g2, rows, :], els.at[s], ers.at[s],
            )[n]
            landed(dst, swap_recv.at[n, s])

    def z_gather(buf, bank, fine=False):
        def at(dz, half, k=core):
            zz = (z + dz + NZ) % NZ
            if fine:
                return buf.at[zz, pl.ds(k * 8 + half * 4, 4)]
            return buf.at[zz * 2 + k, pl.ds(half * H, H), :]

        def last(way, half):
            return 4 if (way == 1) == (half == 0) else 3

        def slot(way, half, step):
            return z_recv.at[bank, (0 if way == 1 else 8) + half * 4 + step - 1]

        def push(dz, half, way, step):
            ref = at(dz, half)
            remote(ref, ref, z_send.at[bank], slot(way, half, step), dev(dz=way)).start()

        def across(dz, half):
            ref = at(dz, half)
            remote(ref, ref, z_send.at[bank], z_recv.at[bank, 16 + (dz % NZ) * 2 + half], sibling).start()

        def begin():
            for half in (0, 1):
                push(0, half, 1, 1)
                push(0, 1 - half, -1, 1)
            for half in (0, 1):
                across(0, half)

        def arrive(way, half, step):
            landed(at(-way * step, half), slot(way, half, step))
            if step < last(way, half):
                push(-way * step, half, way, step + 1)
            across(-way * step, half)

        events = []
        for way in (1, -1):
            for half in (0, 1):
                for step in range(1, last(way, half) + 1):
                    first = (way == 1) == (half == 0)
                    when = (2 * step - (1 if first else 0)) * 3.2 + 2.2
                    events.append((when, lambda w=way, h=half, s=step: arrive(w, h, s)))

        def crossed(dz):
            for half in (0, 1):
                landed(at(dz, half, 1 - core), z_recv.at[bank, 16 + dz % NZ * 2 + half])

        def sent():
            landed(cs.at[pl.ds(0, 15)], z_send.at[bank])

        def finish():
            for dz in range(NZ):
                crossed(dz)
            sent()

        return begin, events, finish, crossed, sent

    def xy_gather(buf, bank):
        events, begins = [], [[], []]
        for part in (0, 1):
            base = part * H

            def at(i, j, lo=0, n=H, part=part, base=base):
                dy, dx = (j, i) if part == 0 else (i, j)
                return buf.at[((y + dy + NY) % NY) * 4 + (x + dx + NX) % NX, pl.ds(base + lo, n), :]

            def slot(kind, i, way, hop, part=part):
                return xy_recv.at[bank, part * 20 + (kind + (i % 4 if kind else 0)) * 4 + (0 if way == 1 else 2) + hop - 1]

            def along(axis, way, part=part):
                return dev(dx=way) if (axis == 0) == (part == 0) else dev(dy=way)

            def push(ref, axis, way, sem, along=along):
                remote(ref, ref, xy_send.at[bank], sem, along(axis, way)).start()

            def second(i, at=at, slot=slot, push=push):
                for way in (1, -1):
                    push(at(i, 0), 1, way, slot(1, i, way, 1))

            def first_start(at=at, slot=slot, push=push):
                for way in (1, -1):
                    push(at(0, 0), 0, way, slot(0, 0, way, 1))

            begins[0].append(first_start)
            begins[1].append(lambda second=second: second(0))

            def first_hop(way, at=at, slot=slot, push=push, second=second):
                landed(at(-way, 0), slot(0, 0, way, 1))
                push(at(-way, 0, 0 if way == 1 else Q, Q), 0, way, slot(0, 0, way, 2))

            def first_far(at=at, slot=slot, second=second):
                for way in (1, -1):
                    landed(at(2, 0, 0 if way == 1 else Q, Q), slot(0, 0, way, 2))
                second(2)

            def second_hop(i, way, at=at, slot=slot, push=push):
                landed(at(i, -way), slot(1, i, way, 1))
                push(at(i, -way, 0 if way == 1 else Q, Q), 1, way, slot(1, i, way, 2))

            def second_far(i, way, at=at, slot=slot):
                landed(at(i, 2, 0 if way == 1 else Q, Q), slot(1, i, way, 2))

            for way in (1, -1):
                events.append((5.60, lambda f=first_hop, w=way: f(w)))
                events.append((5.61 if way == 1 else 5.62, lambda f=second, w=way: f(-w)))
                events.append((8.7, lambda f=second_hop, w=way: f(0, w)))
                events.append((13.4, lambda f=second_hop, w=way: f(-1, w)))
                events.append((16.5, lambda f=second_hop, w=way: f(1, w)))
                events.append((21.2, lambda f=second_hop, w=way: f(2, w)))
                for when, i in ((18.3, 0), (22.8, -1), (24.3, 1), (25.9, 2)):
                    events.append((when, lambda f=second_far, i=i, w=way: f(i, w)))
            events.append((10.4, first_far))

        def begin():
            for stage in begins:
                for start in stage:
                    start()

        def finish():
            landed(buf.at[pl.ds(0, 15)], xy_send.at[bank])

        return begin, events, finish

    def xy_sum(ready):
        events = []
        for n, dz in enumerate((0, -1, 1, -2, 2, -3, 3, 4)):
            part, way = n % 2, 1 if n // 2 % 2 == 0 else -1
            zc = (z + dz + NZ) % NZ
            me = y if part == 0 else x

            def slab(i, part=part, zc=zc):
                if part == 0:
                    return hp.at[zc, :, (x + i + NX) % NX]
                return hp.at[zc, (y + i + NY) % NY]

            def push(src, dst, what, axis, to, part=part, n=n):
                device = dev(dx=to) if (axis == 0) == (part == 0) else dev(dy=to)
                remote(src, dst, rs_send, rs_recv.at[n, what], device).start()

            def begin(dz=dz, zc=zc, n=n, way=way, slab=slab, push=push):
                ready(dz)

                @pl.loop(0, 2)
                def _(k):
                    part = lax.dot_general(
                        ss[2 * zc + k], qas[g1], (((1,), (1,)), ((), ())), preferred_element_type=jnp.float32
                    )
                    hp[zc, pl.ds(2 * k, 2)] = part.astype(jnp.bfloat16).reshape(2, 4, R, B)

                push(slab(2), rs_t.at[n], 0, 0, way)
                push(slab(-way), rs_b.at[n], 1, 0, -way)

            def relay(n=n, way=way, slab=slab, push=push):
                landed(rs_t.at[n], rs_recv.at[n, 0])
                ref = slab(way)
                for j in range(4):
                    ref[j] = (ref[j].astype(jnp.float32) + rs_t[n, j].astype(jnp.float32)).astype(jnp.bfloat16)
                push(ref, rs_a.at[n], 2, 0, way)

            def middle(n=n, way=way, slab=slab, push=push, me=me):
                landed(rs_b.at[n], rs_recv.at[n, 1])
                landed(rs_a.at[n], rs_recv.at[n, 2])
                ref = slab(0)
                for j in range(4):
                    total = ref[j].astype(jnp.float32) + rs_a[n, j].astype(jnp.float32) + rs_b[n, j].astype(jnp.float32)
                    rs_mid[n, j] = total.astype(jnp.bfloat16)
                push(rs_mid.at[n, (me + 2) % 4], rs_t2.at[n], 3, 1, way)
                push(rs_mid.at[n, (me - way + 4) % 4], rs_b2.at[n], 4, 1, -way)

            def relay2(n=n, way=way, push=push, me=me):
                landed(rs_t2.at[n], rs_recv.at[n, 3])
                ref = rs_mid.at[n, (me + way + 4) % 4]
                ref[...] = (ref[...].astype(jnp.float32) + rs_t2[n].astype(jnp.float32)).astype(jnp.bfloat16)
                push(ref, rs_a2.at[n], 5, 1, way)

            def last(n=n, me=me, zc=zc):
                landed(rs_b2.at[n], rs_recv.at[n, 4])
                landed(rs_a2.at[n], rs_recv.at[n, 5])
                total = rs_mid[n, me].astype(jnp.float32) + rs_a2[n].astype(jnp.float32) + rs_b2[n].astype(jnp.float32)
                h_own[zc] = total.astype(jnp.bfloat16)

            when = (1.5, 9.9, 10.0, 16.3, 16.4, 22.7, 22.8, 25.9)[n]
            for later, event in zip((0.0, 6.4, 12.6, 16.2), (begin, relay, middle, relay2)):
                events.append((when + later, event))
            events.append((44.0 + 0.1 * n, last))
        return events

    def run(*plans):
        for _, event in sorted((e for plan in plans for e in plan), key=lambda e: e[0]):
            event()

    def product(a, b, rows=slice(None)):
        def four(k):
            wide = jnp.concatenate([a[k + n, rows, :] for n in range(4)], axis=1)
            return jnp.dot(wide, b(k), preferred_element_type=jnp.float32)

        acc[rows, :] = four(0)

        @pl.loop(1, 4)
        def _(k):
            acc[rows, :] += four(4 * k)

    exchange(first_pieces, swap_send, swap_recv, "start", (0, 1))
    qa_plan, c_plan = z_gather(qas, 0), xy_gather(cs, 0)
    first_landed(0)
    qa_plan[0]()
    first_landed(1)
    c_plan[0]()
    late = lambda: exchange(first_pieces, swap_send, swap_recv, "start", (2, 3, 4))
    run(qa_plan[1], c_plan[1], [(18.1, late)])
    qa_plan[2]()
    c_plan[2]()

    def rows_of(ref):
        return lambda k: ref[pl.ds(k, 4)].reshape(4 * B, B)

    product(cs, rows_of(qas))
    ps[g1] = acc[...].astype(jnp.bfloat16)
    p_plan, qb_plan = z_gather(ps, 1), xy_gather(qbs, 1)
    p_plan[0]()
    first_landed(2)
    qb_plan[0]()
    first_landed(3)
    first_landed(4)
    diagonal = lax.broadcasted_iota(jnp.int32, (H, H), 0) == lax.broadcasted_iota(jnp.int32, (H, H), 1)
    for s in (0, 1):
        column = jnp.sum(jnp.where(diagonal, ers[s], 0.0), axis=1, keepdims=True)
        er_col[pl.ds(s * H, H), :] = jnp.broadcast_to(column, (H, 128))
    qb2[z, pl.ds(core * 8, 8)] = qbs[g2].reshape(8, R, B)
    run(p_plan[1], qb_plan[1])
    exchange(first_pieces, swap_send, swap_recv, "wait")
    p_plan[2]()
    qb_plan[2]()

    product(qbs, rows_of(ps))
    ss[g1] = (acc[...] / (els[0] + er_col[:, 0:1])).astype(jnp.bfloat16)
    s_plan, qb2_plan = z_gather(ss, 0), z_gather(qb2, 1, fine=True)
    s_plan[0]()
    start, cut = 25.0, 39.0
    early = [(t + start, e) for t, e in qb2_plan[1] if t + start <= cut]
    after = [(t + start - cut, e) for t, e in qb2_plan[1] if t + start > cut]
    run(s_plan[1], xy_sum(s_plan[3]), [(start, qb2_plan[0])], early)
    hs[g2] = h_own[...].reshape(B, B).astype(jnp.float32).T.astype(jnp.bfloat16)
    h_plan = xy_gather(hs, 0)
    h_plan[0]()
    s_plan[4]()
    landed(cs.at[pl.ds(0, 15)], rs_send)
    run(h_plan[1], after)
    qb2_plan[2]()
    h_plan[2]()

    def rows_across(k):
        return jnp.concatenate([qb2[:, k + n].reshape(B, B) for n in range(4)], axis=0)

    def last_pieces(h, to_x):
        return ((xo.at[pl.ds(h * H, H), :], xin.at[odd_x]),)

    for h in (0, 1):
        rows = pl.ds(h * H, H)
        product(hs, rows_across, rows)
        xo[rows, :] = acc[rows, :].astype(jnp.bfloat16)
        exchange(last_pieces, fin_send, fin_recv, "start", halves=(h,))
    for s in (0, 1):
        landed(xin.at[s], fin_recv.at[0, s])
        out_ref[:, pl.ds(s * B, B)] = xin[s]
    exchange(last_pieces, fin_send, fin_recv, "wait")


def body(rhs, basis_left, basis_right, eig_left, eig_right):
    strip = pltpu.VMEM((16, B, B), jnp.bfloat16)
    slabs, pieces = pltpu.VMEM((8, 4, R, B), jnp.bfloat16), pltpu.VMEM((8, R, B), jnp.bfloat16)
    dma = pltpu.SemaphoreType.DMA
    return pl.pallas_call(
        kernel,
        out_shape=jax.ShapeDtypeStruct((H, 2 * B), jnp.bfloat16),
        in_specs=[pl.BlockSpec(memory_space=pltpu.VMEM)] * 5,
        out_specs=pl.BlockSpec(memory_space=pltpu.VMEM),
        scratch_shapes=[
            strip, strip, strip, strip, strip,
            pltpu.VMEM((8, 4, 4, R, B), jnp.bfloat16),
            strip,
            pltpu.VMEM((8, 16, R, B), jnp.bfloat16),
            pltpu.VMEM((B, B), jnp.float32),
            pltpu.VMEM((2, 1, B), jnp.float32),
            pltpu.VMEM((2, 1, H), jnp.float32),
            pltpu.VMEM((B, 128), jnp.float32),
            slabs, slabs, slabs, slabs, pieces, pieces, pieces, pieces,
            pltpu.VMEM((B, B), jnp.bfloat16),
            pltpu.VMEM((2, H, B), jnp.bfloat16),
            dma((5, 2)), dma((5, 2)), dma((2, 32)), dma((2, 40)), dma((8, 6)), dma((1, 2)), dma((1, 2)),
            dma((2,)), dma((2,)), dma,
        ],
        compiler_params=pltpu.CompilerParams(
            collective_id=0, has_side_effects=True, vmem_limit_bytes=60 * 1024 * 1024
        ),
    )(
        rhs.T,
        basis_left,
        basis_right.T,
        eig_left[None, :],
        eig_right[None, :],
    )


def solution(mesh):
    in_specs = (P("row", "col"), P("col", "row"), P("row", "col"), P("row"), P("col"))
    out_specs = P("col", "row")
    return jax.shard_map(body, mesh=mesh, in_specs=in_specs, out_specs=out_specs, check_vma=False)
```

```python
import jax
import jax.numpy as jnp
from jax import lax
from jax.experimental import pallas as pl
from jax.experimental.pallas import tpu as pltpu
from jax.sharding import PartitionSpec as P

MESH = pl.DeviceIdType.MESH
B = 384
H = B // 2
Q = B // 4
R = B // 8
NX, NY, NZ = 4, 4, 8
ROUTES = ((1, 1, 1, 1), (1, 1, 0, 1), (0, -1, 1, -1), (1, -1, 0, -1), (0, 1, 1, 1), (1, 1, 0, 1), (0, -1, 1, -1), (1, 1, 0, -1))
ORDER = (0, -1, 1, -2, 2, -3, 3, 4)

WAITS = (
    (
        0, 10, 14, 24, 35, 45, 15, 36, 25, 46, 4, 7, 16, 26, 37, 47, 1, 11, 34, 55, 5, 8, 17, 27, 38, 48, 2, 12, 18,
        28, 39, 49, 6, 9, 19, 29, 40, 50, 56, 3, 13, 20, 30, 41, 51, 21, 31, 42, 52, 22, 32, 43, 53, 23, 33, 44, 54,
    ),
    (
        0, 10, 14, 24, 35, 45, 15, 36, 25, 46, 4, 7, 16, 26, 37, 47, 34, 55, 1, 11, 17, 27, 38, 48, 5, 8, 18, 28,
        39, 49, 2, 12, 19, 29, 40, 50, 6, 9, 3, 13, 20, 30, 41, 51, 21, 31, 42, 52, 22, 32, 43, 53, 23, 33, 44, 54,
    ),
    (
        14, 0, 10, 15, 4, 7, 26, 38, 1, 11, 16, 5, 8, 27, 50, 39, 62, 17, 2, 12, 6, 9, 110, 28, 51, 40, 74, 63, 86,
        18, 3, 13, 29, 98, 52, 111, 121, 41, 64, 75, 87, 115, 118, 53, 19, 21, 99, 30, 65, 112, 122, 88, 22, 54, 23,
        42, 76, 116, 119, 20, 31, 89, 55, 57, 45, 113, 123, 100, 77, 33, 56, 24, 66, 32, 90, 58, 117, 120, 101, 59,
        78, 43, 34, 60, 93, 69, 35, 114, 124, 102, 125, 126, 46, 79, 127, 128, 47, 129, 130, 67, 131, 132, 36, 133,
        25, 44, 91, 103, 61, 81, 80, 105, 70, 71, 48, 92, 94, 82, 106, 95, 83, 107, 104, 68, 49, 37, 96, 72, 108,
        84, 97, 73, 109, 85,
    ),
)


def kernel(
    ct_ref, qa_ref, qbt_ref, el_ref, er_ref, out_ref,
    cs, qas, qbs, ps, ss, hp, hs, qb2, acc, els, ers, er_col,
    rs_t, rs_a, rs_b, rs_mid, rs_t2, rs_a2, rs_b2, xo, xin,
    swap_send, swap_recv, z_recv, xy_recv, rs_recv, ag_recv, fin_send, fin_recv,
    z_send, xy_send, rs_send, ag_send,
):
    r, c = lax.axis_index("row"), lax.axis_index("col")
    y, core, z, x = r // 2, r % 2, c // 4, c % 4
    g1, g2 = z * 2 + core, y * 4 + x

    def dev(dx=0, dy=0, dz=0):
        return {
            "row": ((y + dy + NY) % NY) * 2 + core,
            "col": ((z + dz + NZ) % NZ) * 4 + (x + dx + NX) % NX,
        }

    sibling = {"row": y * 2 + 1 - core, "col": c}

    def remote(src, dst, send, recv, device):
        return pltpu.make_async_remote_copy(
            src_ref=src, dst_ref=dst, send_sem=send, recv_sem=recv,
            device_id=device, device_id_type=MESH,
        )

    def landed(dst, sem):
        pltpu.make_async_copy(dst, dst, sem).wait()

    barrier = pltpu.get_barrier_semaphore()
    greeted = [dev(dy=1), dev(dy=-1), dev(dz=1), dev(dz=-1), sibling]
    for dx in (1, 2, 3):
        for k in (core, 1 - core):
            greeted.append({"row": y * 2 + k, "col": z * 4 + (x + dx) % NX})
    for device in greeted:
        pl.semaphore_signal(barrier, inc=1, device_id=device, device_id_type=MESH)
    pl.semaphore_wait(barrier, len(greeted))

    half_x, odd_x = x // 2, x % 2

    def exchange(pieces, send, recv, act, only=(0, 1, 2, 3, 4)):
        for h in (0, 1):
            to_x = 2 * core + h
            own = jnp.logical_and(to_x == x, half_x == core)
            for n, (src, dst) in enumerate(pieces(h, to_x)):
                if n not in only:
                    continue

                @pl.when(own)
                def _(n=n, src=src, dst=dst):
                    if act == "start":
                        pltpu.make_async_copy(src, dst, recv.at[n, odd_x]).start()

                @pl.when(jnp.logical_not(own))
                def _(n=n, src=src, dst=dst, h=h, to_x=to_x):
                    copy = remote(
                        src, dst, send.at[n, h], recv.at[n, odd_x],
                        {"row": y * 2 + half_x, "col": z * 4 + to_x},
                    )
                    if act == "start":
                        copy.start()
                    else:
                        copy.wait_send()

    def first_pieces(h, to_x):
        lanes = pl.ds(h * B, B)
        rows = pl.ds(pl.multiple_of(odd_x * H, H), H)
        return (
            (qa_ref.at[:, lanes], qas.at[z * 2 + half_x, rows, :]),
            (ct_ref.at[:, lanes], cs.at[y * 4 + to_x, rows, :]),
            (qbt_ref.at[:, lanes], qbs.at[y * 4 + to_x, rows, :]),
            (el_ref, els.at[odd_x]),
            (er_ref, ers.at[odd_x]),
        )

    def first_landed(n):
        for s in (0, 1):
            rows = pl.ds(s * H, H)
            dst = (
                qas.at[g1, rows, :], cs.at[g2, rows, :], qbs.at[g2, rows, :], els.at[s], ers.at[s],
            )[n]
            landed(dst, swap_recv.at[n, s])

    def z_gather(buf, bank, fine=False):
        def at(dz, half, k=core):
            zz = (z + dz + NZ) % NZ
            if fine:
                return buf.at[zz, pl.ds(k * 8 + half * 4, 4)]
            return buf.at[zz * 2 + k, pl.ds(half * H, H), :]

        def last(way, half):
            return 4 if (way == 1) == (half == 0) else 3

        def slot(way, half, step):
            return z_recv.at[bank, (0 if way == 1 else 8) + half * 4 + step - 1]

        def push(dz, half, way, step):
            ref = at(dz, half)
            remote(ref, ref, z_send.at[bank], slot(way, half, step), dev(dz=way)).start()

        def across(dz, half):
            ref = at(dz, half)
            remote(ref, ref, z_send.at[bank], z_recv.at[bank, 16 + (dz % NZ) * 2 + half], sibling).start()

        def begin():
            for half in (0, 1):
                push(0, half, 1, 1)
                push(0, 1 - half, -1, 1)
            for half in (0, 1):
                across(0, half)

        def arrive(way, half, step):
            landed(at(-way * step, half), slot(way, half, step))
            if step < last(way, half):
                push(-way * step, half, way, step + 1)
            across(-way * step, half)

        events = []
        for way in (1, -1):
            for half in (0, 1):
                for step in range(1, last(way, half) + 1):
                    first = (way == 1) == (half == 0)
                    when = (2 * step - (1 if first else 0)) * 3.2 + 2.2
                    events.append((when, lambda w=way, h=half, s=step: arrive(w, h, s)))

        def crossed(dz):
            for half in (0, 1):
                landed(at(dz, half, 1 - core), z_recv.at[bank, 16 + dz % NZ * 2 + half])

        def sent():
            landed(cs.at[pl.ds(0, 15)], z_send.at[bank])

        def finish():
            for dz in range(NZ):
                crossed(dz)
            sent()

        return begin, events, finish, crossed, sent

    def xy_gather(buf, bank):
        events, begins = [], [[], []]
        for part in (0, 1):
            base = part * H

            def at(i, j, lo=0, n=H, part=part, base=base):
                dy, dx = (j, i) if part == 0 else (i, j)
                return buf.at[((y + dy + NY) % NY) * 4 + (x + dx + NX) % NX, pl.ds(base + lo, n), :]

            def slot(kind, i, way, hop, part=part):
                return xy_recv.at[bank, part * 20 + (kind + (i % 4 if kind else 0)) * 4 + (0 if way == 1 else 2) + hop - 1]

            def along(axis, way, part=part):
                return dev(dx=way) if (axis == 0) == (part == 0) else dev(dy=way)

            def push(ref, axis, way, sem, along=along):
                remote(ref, ref, xy_send.at[bank], sem, along(axis, way)).start()

            def second(i, at=at, slot=slot, push=push):
                for way in (1, -1):
                    push(at(i, 0), 1, way, slot(1, i, way, 1))

            def first_start(at=at, slot=slot, push=push):
                for way in (1, -1):
                    push(at(0, 0), 0, way, slot(0, 0, way, 1))

            begins[0].append(first_start)
            begins[1].append(lambda second=second: second(0))

            def first_hop(way, at=at, slot=slot, push=push, second=second):
                landed(at(-way, 0), slot(0, 0, way, 1))
                push(at(-way, 0, 0 if way == 1 else Q, Q), 0, way, slot(0, 0, way, 2))

            def first_far(at=at, slot=slot, second=second):
                for way in (1, -1):
                    landed(at(2, 0, 0 if way == 1 else Q, Q), slot(0, 0, way, 2))
                second(2)

            def second_hop(i, way, at=at, slot=slot, push=push):
                landed(at(i, -way), slot(1, i, way, 1))
                push(at(i, -way, 0 if way == 1 else Q, Q), 1, way, slot(1, i, way, 2))

            def second_far(i, way, at=at, slot=slot):
                landed(at(i, 2, 0 if way == 1 else Q, Q), slot(1, i, way, 2))

            for way in (1, -1):
                events.append((5.60, lambda f=first_hop, w=way: f(w)))
                events.append((5.61 if way == 1 else 5.62, lambda f=second, w=way: f(-w)))
                events.append((8.7, lambda f=second_hop, w=way: f(0, w)))
                events.append((13.4, lambda f=second_hop, w=way: f(-1, w)))
                events.append((16.5, lambda f=second_hop, w=way: f(1, w)))
                events.append((21.2, lambda f=second_hop, w=way: f(2, w)))
                for when, i in ((18.3, 0), (22.8, -1), (24.3, 1), (25.9, 2)):
                    events.append((when, lambda f=second_far, i=i, w=way: f(i, w)))
            events.append((10.4, first_far))

        def begin():
            for stage in begins:
                for start in stage:
                    start()

        def finish():
            landed(buf.at[pl.ds(0, 15)], xy_send.at[bank])

        return begin, events, finish

    def xy_sum(ready):
        events = []
        for n, dz in enumerate(ORDER):
            part, way, apart, away = ROUTES[n]
            zc = (z + dz + NZ) % NZ
            me = y if part == 0 else x

            def slab(i, part=part, zc=zc):
                if part == 0:
                    return hp.at[zc, :, (x + i + NX) % NX]
                return hp.at[zc, (y + i + NY) % NY]

            def push(src, dst, what, axis, to, part=part, n=n):
                device = dev(dx=to) if (axis == 0) == (part == 0) else dev(dy=to)
                remote(src, dst, rs_send, rs_recv.at[n, what], device).start()

            def begin(dz=dz, zc=zc, n=n, way=way, slab=slab, push=push):
                ready(dz)

                @pl.loop(0, 2)
                def _(k):
                    part = lax.dot_general(
                        ss[2 * zc + k], qas[g1], (((1,), (1,)), ((), ())), preferred_element_type=jnp.float32
                    )
                    hp[zc, pl.ds(2 * k, 2)] = part.astype(jnp.bfloat16).reshape(2, 4, R, B)

                push(slab(2), rs_t.at[n], 0, 0, way)
                push(slab(-way), rs_b.at[n], 1, 0, -way)

            def relay(n=n, way=way, slab=slab, push=push):
                landed(rs_t.at[n], rs_recv.at[n, 0])
                ref = slab(way)
                for j in range(4):
                    ref[j] = (ref[j].astype(jnp.float32) + rs_t[n, j].astype(jnp.float32)).astype(jnp.bfloat16)
                push(ref, rs_a.at[n], 2, 0, way)

            def middle(n=n, way=way, slab=slab, push=push, me=me):
                landed(rs_b.at[n], rs_recv.at[n, 1])
                landed(rs_a.at[n], rs_recv.at[n, 2])
                ref = slab(0)
                for j in range(4):
                    total = ref[j].astype(jnp.float32) + rs_a[n, j].astype(jnp.float32) + rs_b[n, j].astype(jnp.float32)
                    rs_mid[n, j] = total.astype(jnp.bfloat16)
                push(rs_mid.at[n, (me + 2) % 4], rs_t2.at[n], 3, 1, way)
                push(rs_mid.at[n, (me - way + 4) % 4], rs_b2.at[n], 4, 1, -way)

            def relay2(n=n, way=way, push=push, me=me):
                landed(rs_t2.at[n], rs_recv.at[n, 3])
                ref = rs_mid.at[n, (me + way + 4) % 4]
                ref[...] = (ref[...].astype(jnp.float32) + rs_t2[n].astype(jnp.float32)).astype(jnp.bfloat16)
                push(ref, rs_a2.at[n], 5, 1, way)

            def last(n=n, me=me, zc=zc):
                landed(rs_b2.at[n], rs_recv.at[n, 4])
                landed(rs_a2.at[n], rs_recv.at[n, 5])
                total = rs_mid[n, me].astype(jnp.float32) + rs_a2[n].astype(jnp.float32) + rs_b2[n].astype(jnp.float32)
                hs[g2, n] = total.astype(jnp.bfloat16)

            def at(i, j, part=apart, n=n):
                dy, dx = (j, i) if part == 0 else (i, j)
                return hs.at[((y + dy + NY) % NY) * 4 + (x + dx + NX) % NX, n]

            def share(ref, what, axis, to, part=apart, n=n):
                device = dev(dx=to) if (axis == 0) == (part == 0) else dev(dy=to)
                remote(ref, ref, ag_send, ag_recv.at[n, what], device).start()

            def second(i, n=n, way=away, at=at, share=share):
                share(at(i, 0), 3 + 3 * (i % 4), 1, way)
                share(at(i, 0), 4 + 3 * (i % 4), 1, -way)

            def share0(n=n, way=away, at=at, share=share, last=last, second=second):
                last()
                share(at(0, 0), 0, 0, way)
                share(at(0, 0), 1, 0, -way)
                second(0)

            def share1(n=n, way=away, at=at, share=share, second=second):
                landed(at(-way, 0), ag_recv.at[n, 0])
                share(at(-way, 0), 2, 0, way)
                second(-way)
                landed(at(way, 0), ag_recv.at[n, 1])
                second(way)

            def relay3(i, n=n, way=away, at=at, share=share):
                landed(at(i, -way), ag_recv.at[n, 3 + 3 * (i % 4)])
                share(at(i, -way), 5 + 3 * (i % 4), 1, way)

            def share2(n=n, at=at, second=second):
                landed(at(2, 0), ag_recv.at[n, 2])
                second(2)

            def rest(n=n, way=away, at=at, zc=zc):
                for i in range(4):
                    landed(at(i, way), ag_recv.at[n, 4 + 3 * i])
                    landed(at(i, 2), ag_recv.at[n, 5 + 3 * i])
                wide = jnp.concatenate([ps[2 * zc], ps[2 * zc + 1]], axis=1)
                acc[...] += lax.dot_general(
                    wide, hs[:, n].reshape(2 * B, B), (((1,), (0,)), ((), ())), preferred_element_type=jnp.float32
                )

            when = (1.5, 9.9, 10.0, 16.3, 16.4, 22.7, 22.8, 25.9)[n]
            for later, event in zip((0.0, 6.4, 12.6, 16.2), (begin, relay, middle, relay2)):
                events.append((when + later, event))
            when = (34.0, 36.0, 36.1, 40.0, 40.1, 44.5, 44.6, 46.5)[n]
            for later, event in zip((0.0, 4.4, 8.8), (share0, share1, share2)):
                events.append((when + later, event))
            for later, i in ((4.6, 0), (9.0, -away), (9.1, away), (13.2, 2)):
                events.append((when + later, lambda f=relay3, i=i: f(i)))
            events.append((70.0 + 0.1 * n, rest))
        return events

    def run(order, *plans):
        events = [event for plan in plans for _, event in plan]
        assert sorted(order) == list(range(len(events)))
        for n in order:
            events[n]()

    def product(a, b):
        def four(k):
            wide = jnp.concatenate([a[k + n] for n in range(4)], axis=1)
            return jnp.dot(wide, b(k), preferred_element_type=jnp.float32)

        acc[...] = four(0)

        @pl.loop(1, 4)
        def _(k):
            acc[...] += four(4 * k)

    exchange(first_pieces, swap_send, swap_recv, "start", (0, 1))
    qa_plan, c_plan = z_gather(qas, 0), xy_gather(cs, 0)
    first_landed(0)
    qa_plan[0]()
    first_landed(1)
    c_plan[0]()
    late = lambda: exchange(first_pieces, swap_send, swap_recv, "start", (2, 3, 4))
    run(WAITS[0], qa_plan[1], c_plan[1], [(21.25, late)])
    qa_plan[2]()
    c_plan[2]()

    def rows_of(ref):
        return lambda k: ref[pl.ds(k, 4)].reshape(4 * B, B)

    product(cs, rows_of(qas))
    ps[g1] = acc[...].astype(jnp.bfloat16)
    p_plan, qb_plan = z_gather(ps, 1), xy_gather(qbs, 1)
    p_plan[0]()
    first_landed(2)
    qb_plan[0]()
    first_landed(3)
    first_landed(4)
    diagonal = lax.broadcasted_iota(jnp.int32, (H, H), 0) == lax.broadcasted_iota(jnp.int32, (H, H), 1)
    for s in (0, 1):
        column = jnp.sum(jnp.where(diagonal, ers[s], 0.0), axis=1, keepdims=True)
        er_col[pl.ds(s * H, H), :] = jnp.broadcast_to(column, (H, 128))
    qb2[z, pl.ds(core * 8, 8)] = qbs[g2].reshape(8, R, B)
    run(WAITS[1], p_plan[1], qb_plan[1])
    exchange(first_pieces, swap_send, swap_recv, "wait")
    p_plan[2]()
    qb_plan[2]()

    product(qbs, rows_of(ps))
    el_row = jnp.concatenate([els[0, pl.ds(3 * odd_x + n, 1), :] for n in range(3)], axis=1)
    ss[g1] = (acc[...] / (el_row + er_col[:, 0:1])).astype(jnp.bfloat16)
    s_plan, qb2_plan = z_gather(ss, 0), z_gather(qb2, 1, fine=True)
    s_plan[0]()
    start = 21.5
    tail = [(start, qb2_plan[0])] + [(t + start, e) for t, e in qb2_plan[1]] + [(51.5, qb2_plan[2])]

    def turn(dz):
        zc = (z + dz + NZ) % NZ
        for k in (0, 1):
            block = qb2[zc, pl.ds(8 * k, 8)].reshape(B, B)
            ps[2 * zc + k] = block.astype(jnp.float32).T.astype(jnp.bfloat16)

    tail += [(51.6 + 0.9 * k, lambda dz=dz: turn(dz)) for k, dz in enumerate(ORDER)]
    acc[...] = jnp.zeros_like(acc)
    run(WAITS[2], s_plan[1], xy_sum(s_plan[3]), tail)
    s_plan[4]()
    landed(cs.at[pl.ds(0, 15)], rs_send)
    landed(cs.at[pl.ds(0, 15)], ag_send)

    for third in range(3):
        lanes = pl.ds(third * 128, 128)
        xo[:, lanes] = acc[lanes, :].T.astype(jnp.bfloat16)

        def last_pieces(h, to_x, lanes=lanes):
            return tuple((xo.at[pl.ds(h * H, H), lanes], xin.at[odd_x, :, lanes]) for _ in range(3))

        exchange(last_pieces, fin_send, fin_recv, "start", (third,))

    def all_pieces(h, to_x):
        cuts = [pl.ds(third * 128, 128) for third in range(3)]
        return tuple((xo.at[pl.ds(h * H, H), lanes], xin.at[odd_x, :, lanes]) for lanes in cuts)

    for third in range(3):
        for s in (0, 1):
            landed(xin.at[s, :, pl.ds(third * 128, 128)], fin_recv.at[third, s])
            out_ref[:, pl.ds(s * B + third * 128, 128)] = xin[s, :, pl.ds(third * 128, 128)]
    exchange(all_pieces, fin_send, fin_recv, "wait")


def body(rhs, basis_left, basis_right, eig_left, eig_right):
    strip = pltpu.VMEM((16, B, B), jnp.bfloat16)
    slabs, pieces = pltpu.VMEM((8, 4, R, B), jnp.bfloat16), pltpu.VMEM((8, R, B), jnp.bfloat16)
    dma = pltpu.SemaphoreType.DMA
    return pl.pallas_call(
        kernel,
        out_shape=jax.ShapeDtypeStruct((H, 2 * B), jnp.bfloat16),
        in_specs=[pl.BlockSpec(memory_space=pltpu.VMEM)] * 5,
        out_specs=pl.BlockSpec(memory_space=pltpu.VMEM),
        scratch_shapes=[
            strip, strip, strip, strip, strip,
            pltpu.VMEM((8, 4, 4, R, B), jnp.bfloat16),
            pltpu.VMEM((16, 8, R, B), jnp.bfloat16),
            pltpu.VMEM((8, 16, R, B), jnp.bfloat16),
            pltpu.VMEM((B, B), jnp.float32),
            pltpu.VMEM((2, 6, 128), jnp.float32),
            pltpu.VMEM((2, 1, H), jnp.float32),
            pltpu.VMEM((B, 128), jnp.float32),
            slabs, slabs, slabs, slabs, pieces, pieces, pieces,
            pltpu.VMEM((B, B), jnp.bfloat16),
            pltpu.VMEM((2, H, B), jnp.bfloat16),
            dma((5, 2)), dma((5, 2)), dma((2, 32)), dma((2, 40)), dma((8, 6)), dma((8, 15)), dma((3, 2)), dma((3, 2)),
            dma((2,)), dma((2,)), dma, dma,
        ],
        compiler_params=pltpu.CompilerParams(
            collective_id=0, has_side_effects=True, vmem_limit_bytes=60 * 1024 * 1024
        ),
    )(
        rhs.T,
        basis_left,
        basis_right.T,
        eig_left.reshape(6, 128),
        eig_right[None, :],
    )


def solution(mesh):
    in_specs = (P("row", "col"), P("col", "row"), P("row", "col"), P("row"), P("col"))
    out_specs = P("col", "row")
    return jax.shard_map(body, mesh=mesh, in_specs=in_specs, out_specs=out_specs, check_vma=False)
```

```python
import jax
import jax.numpy as jnp
from jax import lax
from jax.experimental import pallas as pl
from jax.experimental.pallas import tpu as pltpu
from jax.sharding import PartitionSpec as P

MESH = pl.DeviceIdType.MESH
B = 384
H = B // 2
Q = B // 4
R = B // 8
NX, NY, NZ = 4, 4, 8
ROUTES = ((1, 1, 1, 1), (1, 1, 0, 1), (0, -1, 1, -1), (1, -1, 0, -1), (0, 1, 1, 1), (1, 1, 0, 1), (0, -1, 1, -1), (1, 1, 0, -1))
ORDER = (0, -1, 1, -2, 2, -3, 3, 4)

WAITS = (
    (
        0, 10, 14, 24, 35, 45, 15, 36, 25, 46, 4, 7, 16, 26, 37, 47, 1, 11, 34, 55, 5, 8, 17, 27, 38, 48, 2, 12, 18,
        28, 39, 49, 6, 9, 19, 29, 40, 50, 56, 3, 13, 20, 30, 41, 51, 21, 31, 42, 52, 22, 32, 43, 53, 23, 33, 44, 54,
    ),
    (
        0, 10, 14, 24, 35, 45, 15, 36, 25, 46, 4, 7, 16, 26, 37, 47, 34, 55, 1, 11, 17, 27, 38, 48, 5, 8, 18, 28,
        39, 49, 2, 12, 19, 29, 40, 50, 6, 9, 3, 13, 20, 30, 41, 51, 21, 31, 42, 52, 22, 32, 43, 53, 23, 33, 44, 54,
    ),
    (
        14, 0, 10, 15, 4, 7, 26, 38, 1, 11, 16, 5, 8, 27, 50, 39, 62, 17, 2, 12, 6, 9, 110, 28, 51, 40, 74, 63, 86,
        18, 3, 13, 29, 98, 52, 111, 121, 41, 64, 75, 87, 115, 118, 53, 19, 21, 99, 30, 65, 112, 122, 88, 22, 54, 23,
        42, 76, 116, 119, 20, 31, 89, 55, 57, 45, 113, 123, 100, 77, 33, 56, 24, 66, 32, 90, 58, 117, 120, 101, 59,
        78, 43, 34, 60, 93, 69, 35, 114, 124, 102, 125, 126, 46, 79, 127, 128, 47, 129, 130, 67, 131, 132, 36, 133,
        25, 44, 91, 103, 61, 81, 80, 105, 70, 71, 48, 92, 94, 82, 106, 95, 83, 107, 104, 68, 49, 37, 96, 72, 108,
        84, 97, 73, 109, 85,
    ),
)


def kernel(
    ct_in, qa_in, qbt_in, el_ref, er_ref, out_ref,
    ct_ref, qa_ref, qbt_ref,
    cs, qas, qbs, ps, ss, hp, hs, qb2, acc, els, ers, er_col,
    rs_t, rs_a, rs_b, rs_mid, rs_t2, rs_a2, rs_b2, xo, xin,
    swap_send, swap_recv, z_recv, xy_recv, rs_recv, ag_recv, fin_send, fin_recv,
    z_send, xy_send, rs_send, ag_send, in_sem,
):
    r, c = lax.axis_index("row"), lax.axis_index("col")
    y, core, z, x = r // 2, r % 2, c // 4, c % 4
    g1, g2 = z * 2 + core, y * 4 + x

    def dev(dx=0, dy=0, dz=0):
        return {
            "row": ((y + dy + NY) % NY) * 2 + core,
            "col": ((z + dz + NZ) % NZ) * 4 + (x + dx + NX) % NX,
        }

    sibling = {"row": y * 2 + 1 - core, "col": c}

    def remote(src, dst, send, recv, device):
        return pltpu.make_async_remote_copy(
            src_ref=src, dst_ref=dst, send_sem=send, recv_sem=recv,
            device_id=device, device_id_type=MESH,
        )

    def landed(dst, sem):
        pltpu.make_async_copy(dst, dst, sem).wait()

    loads = [
        pltpu.make_async_copy(src, dst, in_sem.at[n])
        for n, (src, dst) in enumerate(((qa_in, qa_ref), (ct_in, ct_ref), (qbt_in, qbt_ref)))
    ]
    for load in loads:
        load.start()

    barrier = pltpu.get_barrier_semaphore()
    greeted = [dev(dy=1), dev(dy=-1), dev(dz=1), dev(dz=-1), sibling]
    for dx in (1, 2, 3):
        for k in (core, 1 - core):
            greeted.append({"row": y * 2 + k, "col": z * 4 + (x + dx) % NX})
    for device in greeted:
        pl.semaphore_signal(barrier, inc=1, device_id=device, device_id_type=MESH)
    pl.semaphore_wait(barrier, len(greeted))

    half_x, odd_x = x // 2, x % 2

    def exchange(pieces, send, recv, act, only=(0, 1, 2, 3, 4)):
        for h in (0, 1):
            to_x = 2 * core + h
            own = jnp.logical_and(to_x == x, half_x == core)
            for n, (src, dst) in enumerate(pieces(h, to_x)):
                if n not in only:
                    continue

                @pl.when(own)
                def _(n=n, src=src, dst=dst):
                    if act == "start":
                        pltpu.make_async_copy(src, dst, recv.at[n, odd_x]).start()

                @pl.when(jnp.logical_not(own))
                def _(n=n, src=src, dst=dst, h=h, to_x=to_x):
                    copy = remote(
                        src, dst, send.at[n, h], recv.at[n, odd_x],
                        {"row": y * 2 + half_x, "col": z * 4 + to_x},
                    )
                    if act == "start":
                        copy.start()
                    else:
                        copy.wait_send()

    def first_pieces(h, to_x):
        lanes = pl.ds(h * B, B)
        rows = pl.ds(pl.multiple_of(odd_x * H, H), H)
        return (
            (qa_ref.at[:, lanes], qas.at[z * 2 + half_x, rows, :]),
            (ct_ref.at[:, lanes], cs.at[y * 4 + to_x, rows, :]),
            (qbt_ref.at[:, lanes], qbs.at[y * 4 + to_x, rows, :]),
            (el_ref, els.at[odd_x]),
            (er_ref, ers.at[odd_x]),
        )

    def first_landed(n):
        for s in (0, 1):
            rows = pl.ds(s * H, H)
            dst = (
                qas.at[g1, rows, :], cs.at[g2, rows, :], qbs.at[g2, rows, :], els.at[s], ers.at[s],
            )[n]
            landed(dst, swap_recv.at[n, s])

    def z_gather(buf, bank, fine=False):
        def at(dz, half, k=core):
            zz = (z + dz + NZ) % NZ
            if fine:
                return buf.at[zz, pl.ds(k * 8 + half * 4, 4)]
            return buf.at[zz * 2 + k, pl.ds(half * H, H), :]

        def last(way, half):
            return 4 if (way == 1) == (half == 0) else 3

        def slot(way, half, step):
            return z_recv.at[bank, (0 if way == 1 else 8) + half * 4 + step - 1]

        def push(dz, half, way, step):
            ref = at(dz, half)
            remote(ref, ref, z_send.at[bank], slot(way, half, step), dev(dz=way)).start()

        def across(dz, half):
            ref = at(dz, half)
            remote(ref, ref, z_send.at[bank], z_recv.at[bank, 16 + (dz % NZ) * 2 + half], sibling).start()

        def begin():
            for half in (0, 1):
                push(0, half, 1, 1)
                push(0, 1 - half, -1, 1)
            for half in (0, 1):
                across(0, half)

        def arrive(way, half, step):
            landed(at(-way * step, half), slot(way, half, step))
            if step < last(way, half):
                push(-way * step, half, way, step + 1)
            across(-way * step, half)

        events = []
        for way in (1, -1):
            for half in (0, 1):
                for step in range(1, last(way, half) + 1):
                    first = (way == 1) == (half == 0)
                    when = (2 * step - (1 if first else 0)) * 3.2 + 2.2
                    events.append((when, lambda w=way, h=half, s=step: arrive(w, h, s)))

        def crossed(dz):
            for half in (0, 1):
                landed(at(dz, half, 1 - core), z_recv.at[bank, 16 + dz % NZ * 2 + half])

        def sent():
            landed(cs.at[pl.ds(0, 15)], z_send.at[bank])

        def finish():
            for dz in range(NZ):
                crossed(dz)
            sent()

        return begin, events, finish, crossed, sent

    def xy_gather(buf, bank):
        events, begins = [], [[], []]
        for part in (0, 1):
            base = part * H

            def at(i, j, lo=0, n=H, part=part, base=base):
                dy, dx = (j, i) if part == 0 else (i, j)
                return buf.at[((y + dy + NY) % NY) * 4 + (x + dx + NX) % NX, pl.ds(base + lo, n), :]

            def slot(kind, i, way, hop, part=part):
                return xy_recv.at[bank, part * 20 + (kind + (i % 4 if kind else 0)) * 4 + (0 if way == 1 else 2) + hop - 1]

            def along(axis, way, part=part):
                return dev(dx=way) if (axis == 0) == (part == 0) else dev(dy=way)

            def push(ref, axis, way, sem, along=along):
                remote(ref, ref, xy_send.at[bank], sem, along(axis, way)).start()

            def second(i, at=at, slot=slot, push=push):
                for way in (1, -1):
                    push(at(i, 0), 1, way, slot(1, i, way, 1))

            def first_start(at=at, slot=slot, push=push):
                for way in (1, -1):
                    push(at(0, 0), 0, way, slot(0, 0, way, 1))

            begins[0].append(first_start)
            begins[1].append(lambda second=second: second(0))

            def first_hop(way, at=at, slot=slot, push=push, second=second):
                landed(at(-way, 0), slot(0, 0, way, 1))
                push(at(-way, 0, 0 if way == 1 else Q, Q), 0, way, slot(0, 0, way, 2))

            def first_far(at=at, slot=slot, second=second):
                for way in (1, -1):
                    landed(at(2, 0, 0 if way == 1 else Q, Q), slot(0, 0, way, 2))
                second(2)

            def second_hop(i, way, at=at, slot=slot, push=push):
                landed(at(i, -way), slot(1, i, way, 1))
                push(at(i, -way, 0 if way == 1 else Q, Q), 1, way, slot(1, i, way, 2))

            def second_far(i, way, at=at, slot=slot):
                landed(at(i, 2, 0 if way == 1 else Q, Q), slot(1, i, way, 2))

            for way in (1, -1):
                events.append((5.60, lambda f=first_hop, w=way: f(w)))
                events.append((5.61 if way == 1 else 5.62, lambda f=second, w=way: f(-w)))
                events.append((8.7, lambda f=second_hop, w=way: f(0, w)))
                events.append((13.4, lambda f=second_hop, w=way: f(-1, w)))
                events.append((16.5, lambda f=second_hop, w=way: f(1, w)))
                events.append((21.2, lambda f=second_hop, w=way: f(2, w)))
                for when, i in ((18.3, 0), (22.8, -1), (24.3, 1), (25.9, 2)):
                    events.append((when, lambda f=second_far, i=i, w=way: f(i, w)))
            events.append((10.4, first_far))

        def begin():
            for stage in begins:
                for start in stage:
                    start()

        def finish():
            landed(buf.at[pl.ds(0, 15)], xy_send.at[bank])

        return begin, events, finish

    def xy_sum(ready):
        events = []
        for n, dz in enumerate(ORDER):
            part, way, apart, away = ROUTES[n]
            zc = (z + dz + NZ) % NZ
            me = y if part == 0 else x

            def slab(i, part=part, zc=zc):
                if part == 0:
                    return hp.at[zc, :, (x + i + NX) % NX]
                return hp.at[zc, (y + i + NY) % NY]

            def push(src, dst, what, axis, to, part=part, n=n):
                device = dev(dx=to) if (axis == 0) == (part == 0) else dev(dy=to)
                remote(src, dst, rs_send, rs_recv.at[n, what], device).start()

            def begin(dz=dz, zc=zc, n=n, way=way, slab=slab, push=push):
                ready(dz)

                @pl.loop(0, 2)
                def _(k):
                    part = lax.dot_general(
                        ss[2 * zc + k], qas[g1], (((1,), (1,)), ((), ())), preferred_element_type=jnp.float32
                    )
                    hp[zc, pl.ds(2 * k, 2)] = part.astype(jnp.bfloat16).reshape(2, 4, R, B)

                push(slab(2), rs_t.at[n], 0, 0, way)
                push(slab(-way), rs_b.at[n], 1, 0, -way)

            def relay(n=n, way=way, slab=slab, push=push):
                landed(rs_t.at[n], rs_recv.at[n, 0])
                ref = slab(way)
                for j in range(4):
                    ref[j] = (ref[j].astype(jnp.float32) + rs_t[n, j].astype(jnp.float32)).astype(jnp.bfloat16)
                push(ref, rs_a.at[n], 2, 0, way)

            def middle(n=n, way=way, slab=slab, push=push, me=me):
                landed(rs_b.at[n], rs_recv.at[n, 1])
                landed(rs_a.at[n], rs_recv.at[n, 2])
                ref = slab(0)
                for j in range(4):
                    total = ref[j].astype(jnp.float32) + rs_a[n, j].astype(jnp.float32) + rs_b[n, j].astype(jnp.float32)
                    rs_mid[n, j] = total.astype(jnp.bfloat16)
                push(rs_mid.at[n, (me + 2) % 4], rs_t2.at[n], 3, 1, way)
                push(rs_mid.at[n, (me - way + 4) % 4], rs_b2.at[n], 4, 1, -way)

            def relay2(n=n, way=way, push=push, me=me):
                landed(rs_t2.at[n], rs_recv.at[n, 3])
                ref = rs_mid.at[n, (me + way + 4) % 4]
                ref[...] = (ref[...].astype(jnp.float32) + rs_t2[n].astype(jnp.float32)).astype(jnp.bfloat16)
                push(ref, rs_a2.at[n], 5, 1, way)

            def last(n=n, me=me, zc=zc):
                landed(rs_b2.at[n], rs_recv.at[n, 4])
                landed(rs_a2.at[n], rs_recv.at[n, 5])
                total = rs_mid[n, me].astype(jnp.float32) + rs_a2[n].astype(jnp.float32) + rs_b2[n].astype(jnp.float32)
                hs[g2, n] = total.astype(jnp.bfloat16)

            def at(i, j, part=apart, n=n):
                dy, dx = (j, i) if part == 0 else (i, j)
                return hs.at[((y + dy + NY) % NY) * 4 + (x + dx + NX) % NX, n]

            def share(ref, what, axis, to, part=apart, n=n):
                device = dev(dx=to) if (axis == 0) == (part == 0) else dev(dy=to)
                remote(ref, ref, ag_send, ag_recv.at[n, what], device).start()

            def second(i, n=n, way=away, at=at, share=share):
                share(at(i, 0), 3 + 3 * (i % 4), 1, way)
                share(at(i, 0), 4 + 3 * (i % 4), 1, -way)

            def share0(n=n, way=away, at=at, share=share, last=last, second=second):
                last()
                share(at(0, 0), 0, 0, way)
                share(at(0, 0), 1, 0, -way)
                second(0)

            def share1(n=n, way=away, at=at, share=share, second=second):
                landed(at(-way, 0), ag_recv.at[n, 0])
                share(at(-way, 0), 2, 0, way)
                second(-way)
                landed(at(way, 0), ag_recv.at[n, 1])
                second(way)

            def relay3(i, n=n, way=away, at=at, share=share):
                landed(at(i, -way), ag_recv.at[n, 3 + 3 * (i % 4)])
                share(at(i, -way), 5 + 3 * (i % 4), 1, way)

            def share2(n=n, at=at, second=second):
                landed(at(2, 0), ag_recv.at[n, 2])
                second(2)

            def rest(n=n, way=away, at=at, zc=zc):
                for i in range(4):
                    landed(at(i, way), ag_recv.at[n, 4 + 3 * i])
                    landed(at(i, 2), ag_recv.at[n, 5 + 3 * i])
                wide = jnp.concatenate([ps[2 * zc], ps[2 * zc + 1]], axis=1)
                acc[...] += lax.dot_general(
                    wide, hs[:, n].reshape(2 * B, B), (((1,), (0,)), ((), ())), preferred_element_type=jnp.float32
                )

            when = (1.5, 9.9, 10.0, 16.3, 16.4, 22.7, 22.8, 25.9)[n]
            for later, event in zip((0.0, 6.4, 12.6, 16.2), (begin, relay, middle, relay2)):
                events.append((when + later, event))
            when = (34.0, 36.0, 36.1, 40.0, 40.1, 44.5, 44.6, 46.5)[n]
            for later, event in zip((0.0, 4.4, 8.8), (share0, share1, share2)):
                events.append((when + later, event))
            for later, i in ((4.6, 0), (9.0, -away), (9.1, away), (13.2, 2)):
                events.append((when + later, lambda f=relay3, i=i: f(i)))
            events.append((70.0 + 0.1 * n, rest))
        return events

    def run(order, *plans):
        events = [event for plan in plans for _, event in plan]
        assert sorted(order) == list(range(len(events)))
        for n in order:
            events[n]()

    def product(a, b):
        def four(k):
            wide = jnp.concatenate([a[k + n] for n in range(4)], axis=1)
            return jnp.dot(wide, b(k), preferred_element_type=jnp.float32)

        acc[...] = four(0)

        @pl.loop(1, 4)
        def _(k):
            acc[...] += four(4 * k)

    for n in (0, 1):
        loads[n].wait()
        exchange(first_pieces, swap_send, swap_recv, "start", (n,))
    loads[2].wait()
    qa_plan, c_plan = z_gather(qas, 0), xy_gather(cs, 0)
    first_landed(0)
    qa_plan[0]()
    first_landed(1)
    c_plan[0]()
    late = lambda: exchange(first_pieces, swap_send, swap_recv, "start", (2, 3, 4))
    run(WAITS[0], qa_plan[1], c_plan[1], [(21.25, late)])
    qa_plan[2]()
    c_plan[2]()

    def rows_of(ref):
        return lambda k: ref[pl.ds(k, 4)].reshape(4 * B, B)

    product(cs, rows_of(qas))
    ps[g1] = acc[...].astype(jnp.bfloat16)
    p_plan, qb_plan = z_gather(ps, 1), xy_gather(qbs, 1)
    p_plan[0]()
    first_landed(2)
    qb_plan[0]()
    first_landed(3)
    first_landed(4)
    diagonal = lax.broadcasted_iota(jnp.int32, (H, H), 0) == lax.broadcasted_iota(jnp.int32, (H, H), 1)
    for s in (0, 1):
        column = jnp.sum(jnp.where(diagonal, ers[s], 0.0), axis=1, keepdims=True)
        er_col[pl.ds(s * H, H), :] = jnp.broadcast_to(column, (H, 128))
    qb2[z, pl.ds(core * 8, 8)] = qbs[g2].reshape(8, R, B)
    run(WAITS[1], p_plan[1], qb_plan[1])
    exchange(first_pieces, swap_send, swap_recv, "wait")
    p_plan[2]()
    qb_plan[2]()

    product(qbs, rows_of(ps))
    el_row = jnp.concatenate([els[0, pl.ds(3 * odd_x + n, 1), :] for n in range(3)], axis=1)
    ss[g1] = (acc[...] / (el_row + er_col[:, 0:1])).astype(jnp.bfloat16)
    s_plan, qb2_plan = z_gather(ss, 0), z_gather(qb2, 1, fine=True)
    s_plan[0]()
    start = 21.5
    tail = [(start, qb2_plan[0])] + [(t + start, e) for t, e in qb2_plan[1]] + [(51.5, qb2_plan[2])]

    def turn(dz):
        zc = (z + dz + NZ) % NZ
        for k in (0, 1):
            block = qb2[zc, pl.ds(8 * k, 8)].reshape(B, B)
            ps[2 * zc + k] = block.astype(jnp.float32).T.astype(jnp.bfloat16)

    tail += [(51.6 + 0.9 * k, lambda dz=dz: turn(dz)) for k, dz in enumerate(ORDER)]
    acc[...] = jnp.zeros_like(acc)
    run(WAITS[2], s_plan[1], xy_sum(s_plan[3]), tail)
    s_plan[4]()
    landed(cs.at[pl.ds(0, 15)], rs_send)
    landed(cs.at[pl.ds(0, 15)], ag_send)

    for third in range(3):
        lanes = pl.ds(third * 128, 128)
        xo[:, lanes] = acc[lanes, :].T.astype(jnp.bfloat16)

        def last_pieces(h, to_x, lanes=lanes):
            return tuple((xo.at[pl.ds(h * H, H), lanes], xin.at[odd_x, :, lanes]) for _ in range(3))

        exchange(last_pieces, fin_send, fin_recv, "start", (third,))

    def all_pieces(h, to_x):
        cuts = [pl.ds(third * 128, 128) for third in range(3)]
        return tuple((xo.at[pl.ds(h * H, H), lanes], xin.at[odd_x, :, lanes]) for lanes in cuts)

    for third in range(3):
        for s in (0, 1):
            landed(xin.at[s, :, pl.ds(third * 128, 128)], fin_recv.at[third, s])
            out_ref[:, pl.ds(s * B + third * 128, 128)] = xin[s, :, pl.ds(third * 128, 128)]
    exchange(all_pieces, fin_send, fin_recv, "wait")


def body(rhs, basis_left, basis_right, eig_left, eig_right):
    strip = pltpu.VMEM((16, B, B), jnp.bfloat16)
    block = pltpu.VMEM((H, 2 * B), jnp.bfloat16)
    slabs, pieces = pltpu.VMEM((8, 4, R, B), jnp.bfloat16), pltpu.VMEM((8, R, B), jnp.bfloat16)
    dma = pltpu.SemaphoreType.DMA
    return pl.pallas_call(
        kernel,
        out_shape=jax.ShapeDtypeStruct((H, 2 * B), jnp.bfloat16),
        in_specs=[pl.BlockSpec(memory_space=pl.ANY)] * 3 + [pl.BlockSpec(memory_space=pltpu.VMEM)] * 2,
        out_specs=pl.BlockSpec(memory_space=pltpu.VMEM),
        scratch_shapes=[
            block, block, block,
            strip, strip, strip, strip, strip,
            pltpu.VMEM((8, 4, 4, R, B), jnp.bfloat16),
            pltpu.VMEM((16, 8, R, B), jnp.bfloat16),
            pltpu.VMEM((8, 16, R, B), jnp.bfloat16),
            pltpu.VMEM((B, B), jnp.float32),
            pltpu.VMEM((2, 6, 128), jnp.float32),
            pltpu.VMEM((2, 1, H), jnp.float32),
            pltpu.VMEM((B, 128), jnp.float32),
            slabs, slabs, slabs, slabs, pieces, pieces, pieces,
            pltpu.VMEM((B, B), jnp.bfloat16),
            pltpu.VMEM((2, H, B), jnp.bfloat16),
            dma((5, 2)), dma((5, 2)), dma((2, 32)), dma((2, 40)), dma((8, 6)), dma((8, 15)), dma((3, 2)), dma((3, 2)),
            dma((2,)), dma((2,)), dma, dma, dma((3,)),
        ],
        compiler_params=pltpu.CompilerParams(
            collective_id=0, has_side_effects=True, vmem_limit_bytes=60 * 1024 * 1024
        ),
    )(
        rhs.T,
        basis_left,
        basis_right.T,
        eig_left.reshape(6, 128),
        eig_right[None, :],
    )


def solution(mesh):
    in_specs = (P("row", "col"), P("col", "row"), P("row", "col"), P("row"), P("col"))
    out_specs = P("col", "row")
    return jax.shard_map(body, mesh=mesh, in_specs=in_specs, out_specs=out_specs, check_vma=False)
```

```python
import jax
import jax.numpy as jnp
from jax import lax
from jax.experimental import pallas as pl
from jax.experimental.pallas import tpu as pltpu
from jax.sharding import PartitionSpec as P

MESH = pl.DeviceIdType.MESH
B = 384
H = B // 2
Q = B // 4
R = B // 8
NX, NY, NZ = 4, 4, 8
ROUTES = ((1, 1, 1, 1), (1, 1, 0, 1), (0, -1, 1, -1), (1, -1, 0, -1), (0, 1, 1, 1), (1, 1, 0, 1), (0, -1, 1, -1), (1, 1, 0, -1))
ORDER = (0, -1, 1, -2, 2, -3, 3, 4)

WAITS = (
    (
        0, 10, 14, 24, 35, 45, 15, 36, 25, 46, 4, 7, 16, 26, 37, 47, 1, 11, 34, 55, 5, 8, 17, 27, 38, 48, 2, 12, 18,
        28, 39, 49, 6, 9, 19, 29, 40, 50, 56, 3, 13, 20, 30, 41, 51, 21, 31, 42, 52, 22, 32, 43, 53, 23, 33, 44, 54,
    ),
    (
        0, 10, 14, 24, 35, 45, 15, 36, 25, 46, 4, 7, 16, 26, 37, 47, 34, 55, 1, 11, 17, 27, 38, 48, 5, 8, 18, 28,
        39, 49, 2, 12, 19, 29, 40, 50, 6, 9, 3, 13, 20, 30, 41, 51, 21, 31, 42, 52, 22, 32, 43, 53, 23, 33, 44, 54,
    ),
    (
        14, 0, 10, 15, 4, 7, 26, 38, 1, 11, 16, 5, 8, 27, 50, 39, 62, 17, 2, 12, 6, 9, 110, 28, 51, 40, 74, 63, 86,
        18, 3, 13, 29, 98, 52, 111, 121, 41, 64, 75, 87, 115, 118, 53, 19, 21, 99, 30, 65, 112, 122, 88, 22, 54, 23,
        42, 76, 116, 119, 20, 31, 89, 55, 57, 45, 113, 123, 100, 77, 33, 56, 24, 66, 32, 90, 58, 117, 120, 101, 59,
        78, 43, 34, 60, 93, 69, 35, 114, 124, 102, 125, 126, 46, 79, 127, 128, 47, 129, 130, 67, 131, 132, 36, 133,
        25, 44, 91, 103, 61, 81, 80, 105, 70, 71, 48, 92, 94, 82, 106, 95, 83, 107, 104, 68, 49, 37, 96, 72, 108,
        84, 97, 73, 109, 85,
    ),
)


def kernel(
    ct_in, qa_in, qbt_in, el_ref, er_ref, out_ref,
    ct_ref, qa_ref, qbt_ref,
    cs, qas, qbs, ps, ss, hp, hs, qb2, acc, els, ers, er_col,
    rs_t, rs_a, rs_b, rs_mid, rs_t2, rs_a2, rs_b2, xo, xin,
    swap_send, swap_recv, z_recv, xy_recv, rs_recv, ag_recv, fin_send, fin_recv,
    z_send, xy_send, rs_send, ag_send, in_sem,
):
    r, c = lax.axis_index("row"), lax.axis_index("col")
    y, core, z, x = r // 2, r % 2, c // 4, c % 4
    g1, g2 = z * 2 + core, y * 4 + x

    def dev(dx=0, dy=0, dz=0):
        return {
            "row": ((y + dy + NY) % NY) * 2 + core,
            "col": ((z + dz + NZ) % NZ) * 4 + (x + dx + NX) % NX,
        }

    sibling = {"row": y * 2 + 1 - core, "col": c}

    def remote(src, dst, send, recv, device):
        return pltpu.make_async_remote_copy(
            src_ref=src, dst_ref=dst, send_sem=send, recv_sem=recv,
            device_id=device, device_id_type=MESH,
        )

    def landed(dst, sem):
        pltpu.make_async_copy(dst, dst, sem).wait()

    loads = [
        pltpu.make_async_copy(src, dst, in_sem.at[n])
        for n, (src, dst) in enumerate(((qa_in, qa_ref), (ct_in, ct_ref), (qbt_in, qbt_ref)))
    ]
    for load in loads:
        load.start()

    barrier = pltpu.get_barrier_semaphore()
    greeted = [dev(dy=1), dev(dy=-1), dev(dz=1), dev(dz=-1), sibling]
    for dx in (1, 2, 3):
        for k in (core, 1 - core):
            greeted.append({"row": y * 2 + k, "col": z * 4 + (x + dx) % NX})
    for device in greeted:
        pl.semaphore_signal(barrier, inc=1, device_id=device, device_id_type=MESH)
    pl.semaphore_wait(barrier, len(greeted))

    half_x, odd_x = x // 2, x % 2

    def exchange(pieces, send, recv, act, only=(0, 1, 2, 3, 4)):
        for h in (0, 1):
            to_x = 2 * core + h
            own = jnp.logical_and(to_x == x, half_x == core)
            for n, (src, dst) in enumerate(pieces(h, to_x)):
                if n not in only:
                    continue

                @pl.when(own)
                def _(n=n, src=src, dst=dst):
                    if act == "start":
                        pltpu.make_async_copy(src, dst, recv.at[n, odd_x]).start()

                @pl.when(jnp.logical_not(own))
                def _(n=n, src=src, dst=dst, h=h, to_x=to_x):
                    copy = remote(
                        src, dst, send.at[n, h], recv.at[n, odd_x],
                        {"row": y * 2 + half_x, "col": z * 4 + to_x},
                    )
                    if act == "start":
                        copy.start()
                    else:
                        copy.wait_send()

    def first_pieces(h, to_x):
        lanes = pl.ds(h * B, B)
        rows = pl.ds(pl.multiple_of(odd_x * H, H), H)
        return (
            (qa_ref.at[:, lanes], qas.at[z * 2 + half_x, rows, :]),
            (ct_ref.at[:, lanes], cs.at[y * 4 + to_x, rows, :]),
            (qbt_ref.at[:, lanes], qbs.at[y * 4 + to_x, rows, :]),
            (el_ref, els.at[odd_x]),
            (er_ref, ers.at[odd_x]),
        )

    def first_landed(n):
        for s in (0, 1):
            rows = pl.ds(s * H, H)
            dst = (
                qas.at[g1, rows, :], cs.at[g2, rows, :], qbs.at[g2, rows, :], els.at[s], ers.at[s],
            )[n]
            landed(dst, swap_recv.at[n, s])

    def z_gather(buf, bank, fine=False):
        def at(dz, half, k=core):
            zz = (z + dz + NZ) % NZ
            if fine:
                return buf.at[zz, pl.ds(k * 8 + half * 4, 4)]
            return buf.at[zz * 2 + k, pl.ds(half * H, H), :]

        def last(way, half):
            return 4 if (way == 1) == (half == 0) else 3

        def slot(way, half, step):
            return z_recv.at[bank, (0 if way == 1 else 8) + half * 4 + step - 1]

        def push(dz, half, way, step):
            ref = at(dz, half)
            remote(ref, ref, z_send.at[bank], slot(way, half, step), dev(dz=way)).start()

        def across(dz, half):
            ref = at(dz, half)
            remote(ref, ref, z_send.at[bank], z_recv.at[bank, 16 + (dz % NZ) * 2 + half], sibling).start()

        def begin():
            for half in (0, 1):
                push(0, half, 1, 1)
                push(0, 1 - half, -1, 1)
            for half in (0, 1):
                across(0, half)

        def arrive(way, half, step):
            landed(at(-way * step, half), slot(way, half, step))
            if step < last(way, half):
                push(-way * step, half, way, step + 1)
            across(-way * step, half)

        events = []
        for way in (1, -1):
            for half in (0, 1):
                for step in range(1, last(way, half) + 1):
                    first = (way == 1) == (half == 0)
                    when = (2 * step - (1 if first else 0)) * 3.2 + 2.2
                    events.append((when, lambda w=way, h=half, s=step: arrive(w, h, s)))

        def crossed(dz):
            for half in (0, 1):
                landed(at(dz, half, 1 - core), z_recv.at[bank, 16 + dz % NZ * 2 + half])

        def sent():
            landed(cs.at[pl.ds(0, 15)], z_send.at[bank])

        def finish():
            for dz in range(NZ):
                crossed(dz)
            sent()

        return begin, events, finish, crossed, sent

    def xy_gather(buf, bank):
        events, begins = [], [[], []]
        for part in (0, 1):
            base = part * H

            def at(i, j, lo=0, n=H, part=part, base=base):
                dy, dx = (j, i) if part == 0 else (i, j)
                return buf.at[((y + dy + NY) % NY) * 4 + (x + dx + NX) % NX, pl.ds(base + lo, n), :]

            def slot(kind, i, way, hop, part=part):
                return xy_recv.at[bank, part * 20 + (kind + (i % 4 if kind else 0)) * 4 + (0 if way == 1 else 2) + hop - 1]

            def along(axis, way, part=part):
                return dev(dx=way) if (axis == 0) == (part == 0) else dev(dy=way)

            def push(ref, axis, way, sem, along=along):
                remote(ref, ref, xy_send.at[bank], sem, along(axis, way)).start()

            def second(i, at=at, slot=slot, push=push):
                for way in (1, -1):
                    push(at(i, 0), 1, way, slot(1, i, way, 1))

            def first_start(at=at, slot=slot, push=push):
                for way in (1, -1):
                    push(at(0, 0), 0, way, slot(0, 0, way, 1))

            begins[0].append(first_start)
            begins[1].append(lambda second=second: second(0))

            def first_hop(way, at=at, slot=slot, push=push, second=second):
                landed(at(-way, 0), slot(0, 0, way, 1))
                push(at(-way, 0, 0 if way == 1 else Q, Q), 0, way, slot(0, 0, way, 2))

            def first_far(at=at, slot=slot, second=second):
                for way in (1, -1):
                    landed(at(2, 0, 0 if way == 1 else Q, Q), slot(0, 0, way, 2))
                second(2)

            def second_hop(i, way, at=at, slot=slot, push=push):
                landed(at(i, -way), slot(1, i, way, 1))
                push(at(i, -way, 0 if way == 1 else Q, Q), 1, way, slot(1, i, way, 2))

            def second_far(i, way, at=at, slot=slot):
                landed(at(i, 2, 0 if way == 1 else Q, Q), slot(1, i, way, 2))

            for way in (1, -1):
                events.append((5.60, lambda f=first_hop, w=way: f(w)))
                events.append((5.61 if way == 1 else 5.62, lambda f=second, w=way: f(-w)))
                events.append((8.7, lambda f=second_hop, w=way: f(0, w)))
                events.append((13.4, lambda f=second_hop, w=way: f(-1, w)))
                events.append((16.5, lambda f=second_hop, w=way: f(1, w)))
                events.append((21.2, lambda f=second_hop, w=way: f(2, w)))
                for when, i in ((18.3, 0), (22.8, -1), (24.3, 1), (25.9, 2)):
                    events.append((when, lambda f=second_far, i=i, w=way: f(i, w)))
            events.append((10.4, first_far))

        def begin():
            for stage in begins:
                for start in stage:
                    start()

        def finish():
            landed(buf.at[pl.ds(0, 15)], xy_send.at[bank])

        return begin, events, finish

    def xy_sum(ready):
        events = []
        for n, dz in enumerate(ORDER):
            part, way, apart, away = ROUTES[n]
            zc = (z + dz + NZ) % NZ
            me = y if part == 0 else x

            def slab(i, part=part, zc=zc):
                if part == 0:
                    return hp.at[zc, :, (x + i + NX) % NX]
                return hp.at[zc, (y + i + NY) % NY]

            def push(src, dst, what, axis, to, part=part, n=n):
                device = dev(dx=to) if (axis == 0) == (part == 0) else dev(dy=to)
                remote(src, dst, rs_send, rs_recv.at[n, what], device).start()

            def begin(dz=dz, zc=zc, n=n, way=way, slab=slab, push=push):
                ready(dz)

                @pl.loop(0, 2)
                def _(k):
                    part = lax.dot_general(
                        ss[2 * zc + k], qas[g1], (((1,), (1,)), ((), ())), preferred_element_type=jnp.float32
                    )
                    hp[zc, pl.ds(2 * k, 2)] = part.astype(jnp.bfloat16).reshape(2, 4, R, B)

                push(slab(2), rs_t.at[n], 0, 0, way)
                push(slab(-way), rs_b.at[n], 1, 0, -way)

            def relay(n=n, way=way, slab=slab, push=push):
                landed(rs_t.at[n], rs_recv.at[n, 0])
                ref = slab(way)
                for j in range(4):
                    ref[j] = (ref[j].astype(jnp.float32) + rs_t[n, j].astype(jnp.float32)).astype(jnp.bfloat16)
                push(ref, rs_a.at[n], 2, 0, way)

            def middle(n=n, way=way, slab=slab, push=push, me=me):
                landed(rs_b.at[n], rs_recv.at[n, 1])
                landed(rs_a.at[n], rs_recv.at[n, 2])
                ref = slab(0)
                for j in range(4):
                    total = ref[j].astype(jnp.float32) + rs_a[n, j].astype(jnp.float32) + rs_b[n, j].astype(jnp.float32)
                    rs_mid[n, j] = total.astype(jnp.bfloat16)
                push(rs_mid.at[n, (me + 2) % 4], rs_t2.at[n], 3, 1, way)
                push(rs_mid.at[n, (me - way + 4) % 4], rs_b2.at[n], 4, 1, -way)

            def relay2(n=n, way=way, push=push, me=me):
                landed(rs_t2.at[n], rs_recv.at[n, 3])
                ref = rs_mid.at[n, (me + way + 4) % 4]
                ref[...] = (ref[...].astype(jnp.float32) + rs_t2[n].astype(jnp.float32)).astype(jnp.bfloat16)
                push(ref, rs_a2.at[n], 5, 1, way)

            def last(n=n, me=me, zc=zc):
                landed(rs_b2.at[n], rs_recv.at[n, 4])
                landed(rs_a2.at[n], rs_recv.at[n, 5])
                total = rs_mid[n, me].astype(jnp.float32) + rs_a2[n].astype(jnp.float32) + rs_b2[n].astype(jnp.float32)
                hs[g2, n] = total.astype(jnp.bfloat16)

            def at(i, j, part=apart, n=n):
                dy, dx = (j, i) if part == 0 else (i, j)
                return hs.at[((y + dy + NY) % NY) * 4 + (x + dx + NX) % NX, n]

            def share(ref, what, axis, to, part=apart, n=n):
                device = dev(dx=to) if (axis == 0) == (part == 0) else dev(dy=to)
                remote(ref, ref, ag_send, ag_recv.at[n, what], device).start()

            def second(i, n=n, way=away, at=at, share=share):
                share(at(i, 0), 3 + 3 * (i % 4), 1, way)
                share(at(i, 0), 4 + 3 * (i % 4), 1, -way)

            def share0(n=n, way=away, at=at, share=share, last=last, second=second):
                last()
                share(at(0, 0), 0, 0, way)
                share(at(0, 0), 1, 0, -way)
                second(0)

            def share1(n=n, way=away, at=at, share=share, second=second):
                landed(at(-way, 0), ag_recv.at[n, 0])
                share(at(-way, 0), 2, 0, way)
                second(-way)
                landed(at(way, 0), ag_recv.at[n, 1])
                second(way)

            def relay3(i, n=n, way=away, at=at, share=share):
                landed(at(i, -way), ag_recv.at[n, 3 + 3 * (i % 4)])
                share(at(i, -way), 5 + 3 * (i % 4), 1, way)

            def share2(n=n, at=at, second=second):
                landed(at(2, 0), ag_recv.at[n, 2])
                second(2)

            def rest(n=n, way=away, at=at, zc=zc):
                for i in range(4):
                    landed(at(i, way), ag_recv.at[n, 4 + 3 * i])
                    landed(at(i, 2), ag_recv.at[n, 5 + 3 * i])
                wide = jnp.concatenate([ps[2 * zc], ps[2 * zc + 1]], axis=1)
                acc[...] += lax.dot_general(
                    wide, hs[:, n].reshape(2 * B, B), (((1,), (0,)), ((), ())), preferred_element_type=jnp.float32
                )

            when = (1.5, 9.9, 10.0, 16.3, 16.4, 22.7, 22.8, 25.9)[n]
            for later, event in zip((0.0, 6.4, 12.6, 16.2), (begin, relay, middle, relay2)):
                events.append((when + later, event))
            when = (34.0, 36.0, 36.1, 40.0, 40.1, 44.5, 44.6, 46.5)[n]
            for later, event in zip((0.0, 4.4, 8.8), (share0, share1, share2)):
                events.append((when + later, event))
            for later, i in ((4.6, 0), (9.0, -away), (9.1, away), (13.2, 2)):
                events.append((when + later, lambda f=relay3, i=i: f(i)))
            events.append((70.0 + 0.1 * n, rest))
        return events

    def run(order, *plans):
        events = [event for plan in plans for _, event in plan]
        assert sorted(order) == list(range(len(events)))
        for n in order:
            events[n]()

    def product(a, b):
        def eight(k):
            wide = jnp.concatenate([a[k + n] for n in range(8)], axis=1)
            return jnp.dot(wide, b(k), preferred_element_type=jnp.float32)

        acc[...] = eight(0)
        acc[...] += eight(8)

    for n in (0, 1):
        loads[n].wait()
        exchange(first_pieces, swap_send, swap_recv, "start", (n,))
    loads[2].wait()
    qa_plan, c_plan = z_gather(qas, 0), xy_gather(cs, 0)
    first_landed(0)
    qa_plan[0]()
    first_landed(1)
    c_plan[0]()
    late = lambda: exchange(first_pieces, swap_send, swap_recv, "start", (2, 3, 4))
    run(WAITS[0], qa_plan[1], c_plan[1], [(21.25, late)])
    qa_plan[2]()
    c_plan[2]()

    def rows_of(ref):
        return lambda k: ref[pl.ds(k, 8)].reshape(8 * B, B)

    product(cs, rows_of(qas))
    ps[g1] = acc[...].astype(jnp.bfloat16)
    p_plan, qb_plan = z_gather(ps, 1), xy_gather(qbs, 1)
    p_plan[0]()
    first_landed(2)
    qb_plan[0]()
    first_landed(3)
    first_landed(4)
    diagonal = lax.broadcasted_iota(jnp.int32, (H, H), 0) == lax.broadcasted_iota(jnp.int32, (H, H), 1)
    for s in (0, 1):
        column = jnp.sum(jnp.where(diagonal, ers[s], 0.0), axis=1, keepdims=True)
        er_col[pl.ds(s * H, H), :] = jnp.broadcast_to(column, (H, 128))
    qb2[z, pl.ds(core * 8, 8)] = qbs[g2].reshape(8, R, B)
    run(WAITS[1], p_plan[1], qb_plan[1])
    exchange(first_pieces, swap_send, swap_recv, "wait")
    p_plan[2]()
    qb_plan[2]()

    product(qbs, rows_of(ps))
    el_row = jnp.concatenate([els[0, pl.ds(3 * odd_x + n, 1), :] for n in range(3)], axis=1)
    ss[g1] = (acc[...] / (el_row + er_col[:, 0:1])).astype(jnp.bfloat16)
    s_plan, qb2_plan = z_gather(ss, 0), z_gather(qb2, 1, fine=True)
    s_plan[0]()
    start = 21.5
    tail = [(start, qb2_plan[0])] + [(t + start, e) for t, e in qb2_plan[1]] + [(51.5, qb2_plan[2])]

    def turn(dz):
        zc = (z + dz + NZ) % NZ
        for k in (0, 1):
            block = qb2[zc, pl.ds(8 * k, 8)].reshape(B, B)
            ps[2 * zc + k] = block.astype(jnp.float32).T.astype(jnp.bfloat16)

    tail += [(51.6 + 0.9 * k, lambda dz=dz: turn(dz)) for k, dz in enumerate(ORDER)]
    acc[...] = jnp.zeros_like(acc)
    run(WAITS[2], s_plan[1], xy_sum(s_plan[3]), tail)
    s_plan[4]()
    landed(cs.at[pl.ds(0, 15)], rs_send)
    landed(cs.at[pl.ds(0, 15)], ag_send)

    for third in range(3):
        lanes = pl.ds(third * 128, 128)
        xo[:, lanes] = acc[lanes, :].T.astype(jnp.bfloat16)

        def last_pieces(h, to_x, lanes=lanes):
            return tuple((xo.at[pl.ds(h * H, H), lanes], xin.at[odd_x, :, lanes]) for _ in range(3))

        exchange(last_pieces, fin_send, fin_recv, "start", (third,))

    def all_pieces(h, to_x):
        cuts = [pl.ds(third * 128, 128) for third in range(3)]
        return tuple((xo.at[pl.ds(h * H, H), lanes], xin.at[odd_x, :, lanes]) for lanes in cuts)

    for third in range(3):
        for s in (0, 1):
            landed(xin.at[s, :, pl.ds(third * 128, 128)], fin_recv.at[third, s])
            out_ref[:, pl.ds(s * B + third * 128, 128)] = xin[s, :, pl.ds(third * 128, 128)]
    exchange(all_pieces, fin_send, fin_recv, "wait")


def body(rhs, basis_left, basis_right, eig_left, eig_right):
    strip = pltpu.VMEM((16, B, B), jnp.bfloat16)
    block = pltpu.VMEM((H, 2 * B), jnp.bfloat16)
    slabs, pieces = pltpu.VMEM((8, 4, R, B), jnp.bfloat16), pltpu.VMEM((8, R, B), jnp.bfloat16)
    dma = pltpu.SemaphoreType.DMA
    return pl.pallas_call(
        kernel,
        out_shape=jax.ShapeDtypeStruct((H, 2 * B), jnp.bfloat16),
        in_specs=[pl.BlockSpec(memory_space=pl.ANY)] * 3 + [pl.BlockSpec(memory_space=pltpu.VMEM)] * 2,
        out_specs=pl.BlockSpec(memory_space=pltpu.VMEM),
        scratch_shapes=[
            block, block, block,
            strip, strip, strip, strip, strip,
            pltpu.VMEM((8, 4, 4, R, B), jnp.bfloat16),
            pltpu.VMEM((16, 8, R, B), jnp.bfloat16),
            pltpu.VMEM((8, 16, R, B), jnp.bfloat16),
            pltpu.VMEM((B, B), jnp.float32),
            pltpu.VMEM((2, 6, 128), jnp.float32),
            pltpu.VMEM((2, 1, H), jnp.float32),
            pltpu.VMEM((B, 128), jnp.float32),
            slabs, slabs, slabs, slabs, pieces, pieces, pieces,
            pltpu.VMEM((B, B), jnp.bfloat16),
            pltpu.VMEM((2, H, B), jnp.bfloat16),
            dma((5, 2)), dma((5, 2)), dma((2, 32)), dma((2, 40)), dma((8, 6)), dma((8, 15)), dma((3, 2)), dma((3, 2)),
            dma((2,)), dma((2,)), dma, dma, dma((3,)),
        ],
        compiler_params=pltpu.CompilerParams(
            collective_id=0, has_side_effects=True, vmem_limit_bytes=60 * 1024 * 1024
        ),
    )(
        rhs.T,
        basis_left,
        basis_right.T,
        eig_left.reshape(6, 128),
        eig_right[None, :],
    )


def solution(mesh):
    in_specs = (P("row", "col"), P("col", "row"), P("row", "col"), P("row"), P("col"))
    out_specs = P("col", "row")
    return jax.shard_map(body, mesh=mesh, in_specs=in_specs, out_specs=out_specs, check_vma=False)
```
